32 devices in a mesh: batch: 8 (over y, x, core), heads: 4 (over z).
Axes of the slice: x: 2, y: 2, z: 4, core: 2. Of those that a mesh axis runs over, the one named last changes fastest.
Arguments:
- tokens: bfloat16 [24576, 768], P('batch'), may hold values from -5 to 5
- qkv_weight: bfloat16 [768, 3, 768], P(None, None, 'heads'), may hold values from -0.21875 to 0.21875
- qv_bias: float32 [2, 768], replicated, may hold values from -3 to 3
- conv_weight: float32 [12, 33], replicated, may hold values from -0.875 to 0.875
- out_weight: bfloat16 [768, 768], P('heads'), may hold values from -0.21875 to 0.21875
- out_bias: float32 [768], replicated, may hold values from -1.75 to 1.75
- norm1_gain: float32 [768], replicated, may hold values from 0.5 to 1.5
- norm1_bias: float32 [768], replicated, may hold values from -1.75 to 1.75
- ffn_in_weight: bfloat16 [768, 3072], P(None, ('batch', 'heads')), may hold values from -0.21875 to 0.21875
- ffn_in_bias: bfloat16 [3072], P(('batch', 'heads')), may hold values from -3 to 3
- ffn_out_weight: bfloat16 [3072, 768], P(('batch', 'heads')), may hold values from -0.109375 to 0.109375
- ffn_out_bias: float32 [768], replicated, may hold values from -1.75 to 1.75
- norm2_gain: float32 [768], replicated, may hold values from 0.5 to 1.5
- norm2_bias: float32 [768], replicated, may hold values from -1.75 to 1.75
- cotangent: bfloat16 [24576, 768], P(('batch', 'heads')), may hold values from -12 to 12
- seq_lengths: int32 [24], P('batch'), may hold values from 0 to 3072, as said below
- segment_ids: int32 [24576], P('batch'), may hold values from 0 to 3, as said below
- landmark_bounds: int32 [24, 64], P('batch'), may hold values from 0 to 3024, as said below
Outputs:
- out: bfloat16 [24576, 768], P(('batch', 'heads'))
- input_grad: float32 [24576, 768], P(('batch', 'heads'))
- qkv_weight_grad: float32 [768, 3, 768], P('batch', None, 'heads')
- qv_bias_grad: float32 [2, 768], P(None, 'heads')
- conv_grad: float32 [12, 33], P('heads')
- out_weight_grad: float32 [768, 768], P('heads', 'batch')
- ffn_in_grad: float32 [768, 3072], P(None, ('batch', 'heads'))
- ffn_in_bias_grad: float32 [3072], P(('batch', 'heads'))
- ffn_out_grad: float32 [3072, 768], P(('batch', 'heads'))
- vector_grads: float32 [6, 768], P(None, ('batch', 'heads'))
- condition: float32 [], replicated
The draws below stay inside these ranges and needn't reach their ends.
Inputs may be any that keep to these rules, and one draw needn't show every extreme that they name: `seq_lengths`: each index of batch holds 3 slots: sequences of 1024 to 3072 tokens first, then empty slots of length 0; the lengths of one index sum to at most 3072; at least one index holds a single sequence of 3072 tokens. `segment_ids`: the live tokens of an index of batch lie in order of slot from its first token slot on, each slot's tokens contiguous; the remaining token slots carry 3. landmark_bounds[s, j] = (j times the length of slot s) // 64.
All inputs are finite; a program needn't handle non-finite values.
Results may differ from the reference program's by a relative error of at most 0.013.
Values may be sent and summed in bfloat16 or wider, within the bound.
A program may use at most 448 MiB of HBM per device.

```python
import math
import jax
import jax.numpy as jnp
from jax import lax

D = 768
H = 12
HEAD_DIM = 64
FF = 3072
LANDMARKS = 64
KERNEL = 33
PINV_ITERS = 6
MINLEN = 1024
MAXLEN = 3072
TOK_DEV = 3072
SEQ_DEV = 3
TOKENS = 24576
N_BATCH = 8


def pack_lengths(key):
    pack_count = TOKENS // TOK_DEV
    base_key = jax.random.fold_in(key, 911)
    key_len, key_whole, key_force = jax.random.split(base_key, 3)
    raw_lengths = jax.random.randint(key_len, (pack_count, SEQ_DEV), MINLEN, MAXLEN // 2 + 1)
    seq_ends = jnp.cumsum(raw_lengths, axis=1)
    lengths = jnp.where(seq_ends <= TOK_DEV, raw_lengths, 0)
    whole_pack = jax.random.randint(key_whole, (pack_count,), 0, 8) == 0
    forced = jax.random.randint(key_force, (), 0, pack_count)
    whole_pack = jnp.logical_or(whole_pack, jnp.arange(pack_count) == forced)
    single = jnp.where(jnp.arange(SEQ_DEV) == 0, MAXLEN, 0)
    lengths = jnp.where(whole_pack[:, None], single[None, :], lengths)
    return lengths.astype(jnp.int32)


def draw_seq_lengths(key, part):
    return pack_lengths(key).reshape(-1)


def draw_segment_ids(key, part):
    lengths = pack_lengths(key)
    seq_ends = jnp.cumsum(lengths, axis=1).astype(jnp.int32)
    places = jnp.arange(TOK_DEV, dtype=jnp.int32)
    slot_ids = jnp.sum((seq_ends[:, None, :] <= places[None, :, None]).astype(jnp.int32), axis=2)
    return slot_ids.reshape(-1).astype(jnp.int32)


def draw_landmark_bounds(key, part):
    lengths = pack_lengths(key)
    marks_at = jnp.arange(LANDMARKS, dtype=jnp.int32)
    bounds = marks_at[None, None, :] * lengths[:, :, None] // LANDMARKS
    return bounds.reshape(-1, LANDMARKS).astype(jnp.int32)


def draw_tokens(key, part):
    key_noise, key_freq, key_phase, key_amp = jax.random.split(jax.random.fold_in(key, 17), 4)
    places = (jnp.arange(TOKENS, dtype=jnp.int32) % TOK_DEV).astype(jnp.float32)[:, None]
    frequency = jnp.exp(jax.random.uniform(key_freq, (D,), minval=math.log(2.0 * math.pi / MAXLEN), maxval=math.log(2.0 * math.pi / 16.0)))
    phase_shift = jax.random.uniform(key_phase, (D,), minval=0.0, maxval=2.0 * math.pi)
    noise_part = 0.8 * jnp.clip(jax.random.normal(key_noise, (TOKENS, D)), -4.0, 4.0)
    amplitude = jax.random.uniform(key_amp, (D,), minval=0.6, maxval=1.2)
    return (noise_part + amplitude[None, :] * jnp.sin(places * frequency[None, :] + phase_shift[None, :])).astype(jnp.bfloat16)


def raised(values, stream_key, source, target, blocks, factor):
    def block_of(axis_at):
        return (jnp.arange(values.shape[axis_at]) // (values.shape[axis_at] // blocks)).reshape((-1,) + (1,) * (values.ndim - 1 - axis_at))

    one_side = jax.random.permutation(stream_key, blocks)[block_of(target)]
    other_side = (block_of(target) + blocks // 2) % blocks
    return jnp.where((block_of(source) == one_side) | (block_of(source) == other_side), factor * values, values)


def level_of(key, shape, cuts, low, largest):
    level, own = 1.0, jax.random.fold_in(key, 6)
    for dim, parts in cuts:
        steps = jnp.exp(jax.random.uniform(jax.random.fold_in(own, dim), (parts,), jnp.float32, low / len(cuts), largest / len(cuts)))
        level = level * jnp.repeat(steps, shape[dim] // parts).reshape([-1 if axis == dim else 1 for axis in range(len(shape))])
    return level


def centred(key, dims, deviation, bound, cuts=(), kind=jnp.bfloat16):
    gain = level_of(key, dims, cuts, -0.22, 0.18) if cuts else 1.0
    entries = jax.random.normal(key, dims, jnp.float32) * deviation * gain
    return jnp.minimum(jnp.maximum(entries, -bound), bound).astype(kind)


def gaussian_with(stream_key, extent, scale, reach, cuts, heavy, held_as=jnp.bfloat16):
    drawn = scale * jax.random.normal(stream_key, extent, jnp.float32)
    if cuts:
        drawn = drawn * level_of(stream_key, extent, cuts, -0.22, 0.18)
    return jnp.clip(raised(drawn, jax.random.fold_in(stream_key, 3), *heavy), -reach, reach).astype(held_as)


def setup_inputs(seed: int = 0) -> dict:
    keys = jax.random.split(jax.random.key(seed), 19)
    tokens = draw_tokens(jax.random.fold_in(keys[18], 71), 0)
    qkv_weight = centred(keys[1], (D, 3, H * HEAD_DIM), D ** -0.5, 0.21875, ((2, 4),))
    qv_bias = centred(keys[2], (2, H * HEAD_DIM), 0.5, 3.0, (), jnp.float32)
    conv_weight = centred(keys[3], (H, KERNEL), 0.15, 0.875, (), jnp.float32)
    out_weight = centred(keys[4], (H * HEAD_DIM, D), (H * HEAD_DIM) ** -0.5, 0.21875, ((0, 4),))
    out_bias = centred(keys[5], (D,), 0.3, 1.75, (), jnp.float32)
    norm1_gain = jnp.clip(1.0 + 0.1 * jax.random.normal(keys[6], (D,), jnp.float32), 0.5, 1.5)
    norm1_bias = centred(keys[7], (D,), 0.3, 1.75, (), jnp.float32)
    ffn_in_weight = centred(keys[8], (D, FF), D ** -0.5, 0.21875, ((1, 32),))
    ffn_in_bias = centred(keys[9], (FF,), 0.5, 3.0, ((0, 32),))
    ffn_out_weight = centred(keys[10], (FF, D), FF ** -0.5, 0.109375, ((0, 32),))
    ffn_out_bias = centred(keys[11], (D,), 0.3, 1.75, (), jnp.float32)
    norm2_gain = jnp.clip(1.0 + 0.1 * jax.random.normal(keys[12], (D,), jnp.float32), 0.5, 1.5)
    norm2_bias = centred(keys[13], (D,), 0.3, 1.75, (), jnp.float32)
    cotangent = gaussian_with(keys[14], (TOKENS, D), 1.0, 12.0, ((0, 32),), (0, 1, 32, 2.75))
    seq_lengths = draw_seq_lengths(jax.random.fold_in(keys[18], 71), 0)
    segment_ids = draw_segment_ids(jax.random.fold_in(keys[18], 71), 0)
    landmark_bounds = draw_landmark_bounds(jax.random.fold_in(keys[18], 71), 0)
    return dict(tokens=tokens, qkv_weight=qkv_weight, qv_bias=qv_bias, conv_weight=conv_weight, out_weight=out_weight, out_bias=out_bias, norm1_gain=norm1_gain, norm1_bias=norm1_bias, ffn_in_weight=ffn_in_weight, ffn_in_bias=ffn_in_bias, ffn_out_weight=ffn_out_weight, ffn_out_bias=ffn_out_bias, norm2_gain=norm2_gain, norm2_bias=norm2_bias, cotangent=cotangent, seq_lengths=seq_lengths, segment_ids=segment_ids, landmark_bounds=landmark_bounds)


best_precision = lax.Precision.HIGHEST
mask_fill = -1000000000.0
norm_eps = 1e-05

@jax.custom_vjp
def low(v):
    return lax.optimization_barrier(v.astype(jnp.bfloat16)).astype(jnp.float32)

@jax.custom_vjp
def low_back(v):
    return v

def low_keep(v):
    return (low(v), None)

def low_pass(kept, grad):
    return (grad,)

def back_keep(v):
    return (v, None)

def back_low(kept, grad):
    return (low(grad),)
low.defvjp(low_keep, low_pass)
low_back.defvjp(back_keep, back_low)

def layer_norm(row_data, gain_vec, shift_vec):
    centre = row_data - lax.optimization_barrier(jnp.mean(row_data, axis=1, keepdims=True))
    spread = lax.optimization_barrier(jnp.mean(centre * centre, axis=1, keepdims=True))
    return centre * lax.rsqrt(spread + norm_eps) * gain_vec[None, :] + shift_vec[None, :]

def gelu_exact(values):
    return jax.nn.gelu(values, approximate=False)

def pack_layout(lengths, slot_ids, bounds):
    slot_count = lengths.shape[0]
    tok_count = slot_ids.shape[0]
    mark_count = bounds.shape[1]
    starts = (jnp.cumsum(lengths) - lengths).astype(jnp.int32)
    slot_hit = slot_ids[:, None] == jnp.arange(slot_count, dtype=jnp.int32)[None, :]
    tok_start = lax.optimization_barrier(jnp.sum(jnp.where(slot_hit, starts[None, :], 0), axis=1)).astype(jnp.int32)
    position = jnp.arange(tok_count, dtype=jnp.int32) - tok_start
    tok_bounds = lax.optimization_barrier(jnp.sum(jnp.where(slot_hit[:, :, None], bounds[None, :, :], 0), axis=1)).astype(jnp.int32)
    mark_index = lax.optimization_barrier(jnp.sum((tok_bounds <= position[:, None]).astype(jnp.int32), axis=1)).astype(jnp.int32) - 1
    mark_id = slot_ids * mark_count + mark_index
    all_marks = slot_count * mark_count
    member = (jnp.arange(all_marks, dtype=jnp.int32)[:, None] == mark_id[None, :]).astype(jnp.float32)
    inv_count = 1.0 / jnp.maximum(lax.optimization_barrier(jnp.sum(member, axis=1)), 1.0)
    same_slot = slot_ids[:, None] == (jnp.arange(all_marks, dtype=jnp.int32) // mark_count)[None, :]
    live_tok = (slot_ids < slot_count).astype(jnp.float32)
    live_slot = (lengths > 0).astype(jnp.float32)
    return (member, inv_count, same_slot, slot_ids, live_tok, live_slot)

def batch_mul(left, right):
    return jnp.einsum('sij,sjk->sik', left, right, precision=best_precision)

def head_mix(q_rows, k_rows, v_rows, conv_taps, layout):
    member, inv_count, same_slot, token_slot, live_tok, live_slot = layout
    slot_count = live_slot.shape[0]
    tok_count, head_dim = q_rows.shape
    mark_count = member.shape[0] // slot_count
    root_scale = head_dim ** (-0.25)
    q_scaled = q_rows * root_scale
    k_scaled = k_rows * root_scale
    q_marks = jnp.dot(member, q_scaled, precision=best_precision) * inv_count[:, None]
    k_marks = jnp.dot(member, k_scaled, precision=best_precision) * inv_count[:, None]
    first_scores = jnp.where(same_slot, jnp.dot(q_scaled, k_marks.T, precision=best_precision), mask_fill)
    first_kernel = jax.nn.softmax(first_scores, axis=1)
    q_blocks = q_marks.reshape(slot_count, mark_count, head_dim)
    k_blocks = k_marks.reshape(slot_count, mark_count, head_dim)
    middle_kernel = jax.nn.softmax(jnp.einsum('sid,sjd->sij', q_blocks, k_blocks, precision=best_precision), axis=2)
    column_sums = lax.optimization_barrier(jnp.sum(middle_kernel, axis=1))
    col_bound = lax.optimization_barrier(jnp.max(column_sums, axis=1))
    inverse = jnp.swapaxes(middle_kernel, 1, 2) / col_bound[:, None, None]
    identity_mat = jnp.eye(mark_count, dtype=jnp.float32)[None, :, :]
    for sweep_index in range(PINV_ITERS):
        product = batch_mul(middle_kernel, inverse)
        inner_poly = 7.0 * identity_mat - product
        inner_poly = 15.0 * identity_mat - batch_mul(product, inner_poly)
        inner_poly = 13.0 * identity_mat - batch_mul(product, inner_poly)
        inverse = 0.25 * batch_mul(inverse, inner_poly)
    last_scores = jnp.where(same_slot.T, jnp.dot(q_marks, k_scaled.T, precision=best_precision), mask_fill)
    last_kernel = jax.nn.softmax(last_scores, axis=1)
    mark_values = jnp.dot(last_kernel, v_rows, precision=best_precision)
    mixed_marks = jnp.einsum('sij,sjd->sid', inverse, mark_values.reshape(slot_count, mark_count, head_dim), precision=best_precision).reshape(slot_count * mark_count, head_dim)
    attended = jnp.dot(first_kernel, mixed_marks, precision=best_precision)
    half_width = conv_taps.shape[0] // 2
    padded_v = jnp.pad(v_rows, ((half_width, half_width), (0, 0)))
    padded_slot = jnp.pad(token_slot, (half_width, half_width), constant_values=-1)
    convolved = jnp.zeros_like(v_rows)
    for tap_index in range(conv_taps.shape[0]):
        same_seq = (padded_slot[tap_index:tap_index + tok_count] == token_slot).astype(jnp.float32)
        convolved = convolved + conv_taps[tap_index] * padded_v[tap_index:tap_index + tok_count] * same_seq[:, None]
    mixed_rows = (attended + convolved) * live_tok[:, None]
    return (mixed_rows, jnp.sum(col_bound * live_slot))

def heads_mix(layout, q_all, k_all, v_all, conv_all):
    tok_count = q_all.shape[0]
    head_count = conv_all.shape[0]
    head_dim = q_all.shape[1] // head_count

    def split_heads(row_data):
        return jnp.transpose(row_data.reshape(tok_count, head_count, head_dim), (1, 0, 2))

    def one_head(operands):
        return head_mix(operands[0], operands[1], operands[2], operands[3], layout)
    mixed_rows, bound_sums = lax.map(jax.checkpoint(one_head), (split_heads(q_all), split_heads(k_all), split_heads(v_all), conv_all))
    merged = jnp.transpose(mixed_rows, (1, 0, 2)).reshape(tok_count, head_count * head_dim)
    return (merged, jnp.sum(bound_sums))

def reference(tokens, qkv_weight, qv_bias, conv_weight, out_weight, out_bias, norm1_gain, norm1_bias, ffn_in_weight, ffn_in_bias, ffn_out_weight, ffn_out_bias, norm2_gain, norm2_bias, cotangent, seq_lengths, segment_ids, landmark_bounds):
    tok_packs = tokens.astype(jnp.float32).reshape(N_BATCH, TOK_DEV, D)
    length_packs = seq_lengths.reshape(N_BATCH, SEQ_DEV)
    slot_packs = segment_ids.reshape(N_BATCH, TOK_DEV)
    bound_packs = landmark_bounds.reshape(N_BATCH, SEQ_DEV, LANDMARKS)
    params = (qkv_weight.astype(jnp.float32), qv_bias.astype(jnp.float32), conv_weight.astype(jnp.float32), out_weight.astype(jnp.float32), out_bias.astype(jnp.float32), norm1_gain.astype(jnp.float32), norm1_bias.astype(jnp.float32), ffn_in_weight.astype(jnp.float32), ffn_in_bias.astype(jnp.float32), ffn_out_weight.astype(jnp.float32), ffn_out_bias.astype(jnp.float32), norm2_gain.astype(jnp.float32), norm2_bias.astype(jnp.float32))

    def forward(tok_all, qkv_w, qv_b, conv_w, out_w, out_b, gain_one, shift_one, in_w, in_b, down_w, down_b, gain_two, shift_two):

        def pack_step(totals, pack_item):
            tok_rows, lengths, slot_ids, bounds = pack_item
            layout = pack_layout(lengths, slot_ids, bounds)
            projected = jnp.dot(tok_rows, qkv_w.reshape(D, 3 * H * HEAD_DIM), precision=best_precision).reshape(TOK_DEV, 3, H * HEAD_DIM)
            bias_rows = jnp.stack([qv_b[0], jnp.zeros_like(qv_b[0]), qv_b[1]])
            qkv_low = low(low_back(projected + bias_rows[None, :, :]))
            mixed_rows, bound_sum = heads_mix(layout, qkv_low[:, 0], qkv_low[:, 1], qkv_low[:, 2], conv_w)
            mixed_low = low(low_back(mixed_rows))
            attn_rows = low_back(jnp.dot(mixed_low, out_w, precision=best_precision) + out_b[None, :])
            norm1_out = layer_norm(tok_rows + attn_rows, gain_one, shift_one)
            pre_act = low_back(jnp.dot(low(norm1_out), in_w, precision=best_precision) + in_b[None, :])
            hidden_low = low(gelu_exact(pre_act))
            ffn_result = low_back(jnp.dot(hidden_low, down_w, precision=best_precision) + down_b[None, :])
            final_out = layer_norm(norm1_out + ffn_result, gain_two, shift_two)
            return (totals + bound_sum, final_out)
        bound_total, outs_packed = lax.scan(jax.checkpoint(pack_step), jnp.zeros((), jnp.float32), (tok_all, length_packs, slot_packs, bound_packs))
        return (outs_packed.reshape(N_BATCH * TOK_DEV, D), bound_total)
    final_out, pullback, bound_total = jax.vjp(forward, tok_packs, *params, has_aux=True)
    gradients = pullback(cotangent.astype(jnp.float32))
    live_total = jnp.sum((seq_lengths > 0).astype(jnp.float32)) * H
    condition = bound_total / live_total
    vector_grads = jnp.stack([gradients[11], gradients[12], gradients[13], gradients[6], gradients[7], gradients[5]])
    return (final_out.astype(jnp.bfloat16), gradients[0].reshape(N_BATCH * TOK_DEV, D), gradients[1], gradients[2], gradients[3], gradients[4], gradients[8], gradients[9], gradients[10], vector_grads, condition)
```

```python
from functools import partial

import jax
import jax.numpy as jnp
from jax import lax
from jax.experimental import pallas as pl
from jax.experimental.pallas import tpu as pltpu
from jax.sharding import PartitionSpec as P

HEAD_DIM = 64
PINV_ITERS = 6
SUB = 256
HALO = 128
f32 = jnp.float32
bf16 = jnp.bfloat16
mask_fill = -1000000000.0
norm_eps = 1e-05
contract_rows = (((0,), (0,)), ((), ()))
contract_cols = (((1,), (1,)), ((), ()))


def mul(a, b, ca, cb):
    return lax.dot_general(a, b, (((ca,), (cb,)), ((), ())), preferred_element_type=f32)


def halves(x):
    high = x.astype(bf16)
    return high, (x - high.astype(f32)).astype(bf16)


def mul3(a, b, ca, cb):
    ah, al = halves(a)
    bh, bl = halves(b)
    return mul(ah, bh, ca, cb) + (mul(ah, bl, ca, cb) + mul(al, bh, ca, cb))


def band_of(row):
    wide = jnp.broadcast_to(row, (2 * SUB, 2 * SUB))
    return pltpu.roll(wide, 0, 1, stride=1, stride_axis=0)[:, :SUB].astype(bf16)


def softmax_down(scores):
    top = jnp.max(scores, axis=0, keepdims=True)
    e = jnp.exp(scores - top)
    return e, 1.0 / jnp.sum(e, axis=0, keepdims=True)


def softmax_across(scores):
    e = jnp.exp(scores - jnp.max(scores, axis=1, keepdims=True))
    return e / jnp.sum(e, axis=1, keepdims=True)


def forward_kernel(len_ref, start_ref, lo_ref, hi_ref, inv_ref, taps_ref, qkv_ref,
                   out_ref, marks_ref, lse_ref, square_ref, newton_ref, bound_ref, padded, band, acc):
    heads = taps_ref.shape[0]
    width = heads * HEAD_DIM
    tokens = qkv_ref.shape[1]
    block = out_ref.shape[2]
    marks = lo_ref.shape[0] // len_ref.shape[0]
    root = HEAD_DIM ** (-0.25)
    at = [slice(h * HEAD_DIM, (h + 1) * HEAD_DIM) for h in range(heads)]
    every = range(heads)

    out_ref[...] = jnp.zeros_like(out_ref)
    bound_ref[...] = jnp.zeros_like(bound_ref)
    padded[:, :HALO] = jnp.zeros((width, HALO), bf16)
    padded[:, HALO + tokens:] = jnp.zeros((width, HALO), bf16)
    padded[:, HALO:HALO + tokens] = qkv_ref[2 * width:, :]
    for h in every:
        band[h] = band_of(taps_ref[h:h + 1, :])

    def per_slot(s, carry):
        count, start = len_ref[s], start_ref[s]

        @pl.when(count > 0)
        def _():
            lo = lo_ref[pl.ds(s * marks, marks), :]
            hi = hi_ref[pl.ds(s * marks, marks), :]
            inv = inv_ref[pl.ds(s, 1), :]
            first, last = start // block, (start + count - 1) // block + 1

            def lanes(i):
                return pl.ds(pl.multiple_of(i * block, block), block)

            def token(i):
                return i * block + lax.broadcasted_iota(jnp.int32, (1, block), 1)

            def live(i):
                t = token(i)
                return (t >= start) & (t < start + count)

            acc[...] = jnp.zeros_like(acc)

            def mark_sums(i, c):
                t = token(i)
                member = ((t >= lo) & (t < hi)).astype(f32).astype(bf16)
                acc[...] += mul(qkv_ref[:2 * width, lanes(i)], member, 1, 1)
                return c

            lax.fori_loop(first, last, mark_sums, 0)
            both = acc[...] * inv * root
            marks_ref[s] = both
            ql = [both[at[h]].T for h in every]
            klt = [both[width + h * HEAD_DIM:width + (h + 1) * HEAD_DIM] for h in every]
            middle = [softmax_across(mul3(ql[h], klt[h], 1, 0)) for h in every]
            bound = [jnp.max(jnp.sum(a, axis=0, keepdims=True), axis=1, keepdims=True) for a in middle]
            bound_ref[...] += sum(bound)

            def sweep(it, inverse):
                product = [mul3(middle[h], inverse[h], 1, 0) for h in every]
                side = [mul3(inverse[h], product[h], 1, 0) for h in every]
                poly = [7.0 * product[h] - mul3(product[h], product[h], 1, 0) for h in every]
                for h in every:
                    newton_ref[s, it, 0, h] = inverse[h]
                    newton_ref[s, it, 1, h] = product[h]
                    newton_ref[s, it, 2, h] = side[h]
                    newton_ref[s, it, 3, h] = poly[h]
                return tuple(
                    0.25 * (13.0 * inverse[h] - 15.0 * side[h] + mul3(side[h], poly[h], 1, 0)) for h in every
                )

            inverse = lax.fori_loop(0, PINV_ITERS, sweep, tuple(middle[h].T / bound[h] for h in every))

            query = [(ql[h] * root).astype(bf16) for h in every]

            def scores(i, h):
                key = qkv_ref[width + h * HEAD_DIM:width + (h + 1) * HEAD_DIM, lanes(i)]
                return jnp.where(live(i), mul(query[h], key, 1, 0), mask_fill)

            def find_top(i, tops):
                return tuple(jnp.maximum(tops[h], jnp.max(scores(i, h), axis=1, keepdims=True)) for h in every)

            tops = lax.fori_loop(first, last, find_top, tuple(jnp.full((marks, 1), mask_fill, f32) for _ in every))

            def gather(i, sums):
                out = []
                for h in every:
                    e = jnp.exp(scores(i, h) - tops[h])
                    value = qkv_ref[2 * width + h * HEAD_DIM:2 * width + (h + 1) * HEAD_DIM, lanes(i)]
                    acc[at[h], :] += mul(e.astype(bf16), value, 1, 1)
                    out.append(sums[h] + jnp.sum(e, axis=1, keepdims=True))
                return tuple(out)

            acc[...] = jnp.zeros_like(acc)
            sums = lax.fori_loop(first, last, gather, tuple(jnp.zeros((marks, 1), f32) for _ in every))
            values = [acc[at[h], :] / sums[h] for h in every]
            mixed = [mul3(inverse[h], values[h], 1, 0) for h in every]
            for h in every:
                lse_ref[s, h] = tops[h] + jnp.log(sums[h])
                square_ref[s, 0, h] = middle[h]
                square_ref[s, 1, h] = inverse[h]
                square_ref[s, 2, h] = values[h]
                square_ref[s, 3, h] = mixed[h]
            mixed_t = [mixed[h].T.astype(bf16) for h in every]
            kl = [(klt[h].T * root).astype(bf16) for h in every]

            def finish(i, c):
                for h in every:
                    e, scale = softmax_down(mul(kl[h], qkv_ref[at[h], lanes(i)], 1, 0))
                    rows = mul(mixed_t[h], e.astype(bf16), 1, 0) * scale
                    conv = []
                    for sub in range(block // SUB):
                        left = i * block + sub * SUB
                        t = left - HALO + lax.broadcasted_iota(jnp.int32, (1, 2 * SUB), 1)
                        near = padded[at[h], pl.ds(pl.multiple_of(left, SUB), 2 * SUB)].astype(f32)
                        near = jnp.where((t >= start) & (t < start + count), near, 0.0).astype(bf16)
                        conv.append(mul(near, band[h], 1, 0))
                    rows = rows + jnp.concatenate(conv, axis=1)
                    rows = jnp.where(live(i), rows, out_ref[i, at[h], :].astype(f32))
                    out_ref[i, at[h], :] = rows.astype(bf16)
                return c

            lax.fori_loop(first, last, finish, 0)

        return carry

    lax.fori_loop(0, len_ref.shape[0], per_slot, 0)


def backward_kernel(len_ref, start_ref, lo_ref, hi_ref, inv_ref, taps_ref, qkv_ref, grad_ref, marks_ref, lse_ref,
                    square_ref, newton_ref, out_ref, sums_ref, conv_ref, padded_v, padded_g, band, acc, small, cross):
    heads = taps_ref.shape[0]
    taps = conv_ref.shape[1]
    width = heads * HEAD_DIM
    tokens = qkv_ref.shape[1]
    blocks, _, block = grad_ref.shape
    marks = lo_ref.shape[0] // len_ref.shape[0]
    root = HEAD_DIM ** (-0.25)
    at = [slice(h * HEAD_DIM, (h + 1) * HEAD_DIM) for h in range(heads)]
    k_at = [slice(width + h * HEAD_DIM, width + (h + 1) * HEAD_DIM) for h in range(heads)]
    v_at = [slice(2 * width + h * HEAD_DIM, 2 * width + (h + 1) * HEAD_DIM) for h in range(heads)]
    every = range(heads)
    subs = range(block // SUB)

    acc[...] = jnp.zeros_like(acc)
    cross[...] = jnp.zeros_like(cross)
    for buf in (padded_v, padded_g):
        buf[:, :HALO] = jnp.zeros((width, HALO), bf16)
        buf[:, HALO + tokens:] = jnp.zeros((width, HALO), bf16)
    padded_v[:, HALO:HALO + tokens] = qkv_ref[2 * width:, :]
    for i in range(blocks):
        padded_g[:, HALO + i * block:HALO + (i + 1) * block] = grad_ref[i]
    for h in every:
        band[h] = band_of(taps_ref[h:h + 1, :])

    def per_slot(s, carry):
        count, start = len_ref[s], start_ref[s]

        @pl.when(count > 0)
        def _():
            lo = lo_ref[pl.ds(s * marks, marks), :]
            hi = hi_ref[pl.ds(s * marks, marks), :]
            inv = inv_ref[pl.ds(s, 1), :]
            first, last = start // block, (start + count - 1) // block + 1

            def lanes(i):
                return pl.ds(pl.multiple_of(i * block, block), block)

            def token(i):
                return i * block + lax.broadcasted_iota(jnp.int32, (1, block), 1)

            def inside(t):
                return (t >= start) & (t < start + count)

            def near(buf, i, sub, h):
                left = i * block + sub * SUB
                t = left - HALO + lax.broadcasted_iota(jnp.int32, (1, 2 * SUB), 1)
                wide = buf[at[h], pl.ds(pl.multiple_of(left, SUB), 2 * SUB)].astype(f32)
                return jnp.where(inside(t), wide, 0.0).astype(bf16)

            both = marks_ref[s]
            qlt = [both[at[h]] for h in every]
            klt = [both[k_at[h]] for h in every]
            middle = [square_ref[s, 0, h] for h in every]
            inverse = [square_ref[s, 1, h] for h in every]
            values = [square_ref[s, 2, h] for h in every]
            mixed = [square_ref[s, 3, h].astype(bf16) for h in every]
            klt_low = [(klt[h] * root).astype(bf16) for h in every]
            kl_low = [(klt[h].T * root).astype(bf16) for h in every]
            small[...] = jnp.zeros_like(small)

            def first_part(i, c):
                on = inside(token(i))
                for h in every:
                    query = qkv_ref[at[h], lanes(i)]
                    grad = jnp.where(on, grad_ref[i, at[h], :].astype(f32), 0.0).astype(bf16)
                    e, scale = softmax_down(mul(kl_low[h], query, 1, 0))
                    weight = e * scale
                    part = weight * mul(mixed[h], grad, 1, 0)
                    delta = (part - weight * jnp.sum(part, axis=0, keepdims=True)).astype(bf16)
                    small[0, h] += mul(weight.astype(bf16), grad, 1, 1)
                    small[1, h] += mul(query, delta, 1, 1)
                    acc[at[h], lanes(i)] += mul(klt_low[h], delta, 1, 0)
                return c

            lax.fori_loop(first, last, first_part, 0)
            grad_mixed = [small[0, h] for h in every]
            grad_values = [mul3(inverse[h], grad_mixed[h], 0, 0) for h in every]
            grad_inverse = tuple(mul3(grad_mixed[h], values[h], 1, 1) for h in every)

            def sweep(step, pair):
                g, grad_a = pair
                it = PINV_ITERS - 1 - step
                new_g, new_a = [], []
                for h in every:
                    z, x = newton_ref[s, it, 0, h], newton_ref[s, it, 1, h]
                    y, w = newton_ref[s, it, 2, h], newton_ref[s, it, 3, h]
                    quarter = 0.25 * g[h]
                    dy = mul3(quarter, w, 1, 1) - 15.0 * quarter
                    dw = mul3(y, quarter, 0, 0)
                    dx = 7.0 * dw - mul3(dw, x, 1, 1) - mul3(x, dw, 0, 0) + mul3(z, dy, 0, 0)
                    new_g.append(13.0 * quarter + mul3(dy, x, 1, 1) + mul3(middle[h], dx, 0, 0))
                    new_a.append(grad_a[h] + mul3(dx, z, 1, 1))
                return tuple(new_g), tuple(new_a)

            grad_start, grad_middle = lax.fori_loop(
                0, PINV_ITERS, sweep, (grad_inverse, tuple(jnp.zeros((marks, marks), f32) for _ in every))
            )
            for h in every:
                column = jnp.sum(middle[h], axis=0, keepdims=True)
                bound = jnp.max(column, axis=1, keepdims=True)
                back = grad_start[h].T / bound
                total = jnp.sum(jnp.sum(back * middle[h], axis=0, keepdims=True), axis=1, keepdims=True)
                hit = (column == bound).astype(f32)
                share = hit * (-total / bound / jnp.sum(hit, axis=1, keepdims=True))
                grad_a = grad_middle[h] + back + share
                delta = middle[h] * (grad_a - jnp.sum(grad_a * middle[h], axis=1, keepdims=True))
                small[2, h] = mul3(klt[h], delta, 1, 1)
                small[3, h] = mul3(qlt[h], delta, 1, 0)
                small[0, h] = jnp.zeros((marks, marks), f32)
            offset = [jnp.sum(grad_values[h] * values[h], axis=1, keepdims=True) for h in every]
            grad_low = [grad_values[h].astype(bf16) for h in every]
            grad_low_t = [grad_values[h].T.astype(bf16) for h in every]
            qlt_low = [(qlt[h] * root).astype(bf16) for h in every]
            ql_low = [(qlt[h].T * root).astype(bf16) for h in every]

            def second_part(i, c):
                on = inside(token(i))
                for h in every:
                    key, value = qkv_ref[k_at[h], lanes(i)], qkv_ref[v_at[h], lanes(i)]
                    score = jnp.where(on, mul(ql_low[h], key, 1, 0), mask_fill)
                    weight = jnp.exp(score - lse_ref[s, h])
                    delta = (weight * (mul(grad_low[h], value, 1, 0) - offset[h])).astype(bf16)
                    small[0, h] += mul(key, delta, 1, 1)
                    acc[k_at[h], lanes(i)] += mul(qlt_low[h], delta, 1, 0)
                    around_g = [near(padded_g, i, sub, h) for sub in subs]
                    around_v = [near(padded_v, i, sub, h) for sub in subs]
                    conv = jnp.concatenate([mul(g, band[h], 1, 0) for g in around_g], axis=1)
                    acc[v_at[h], lanes(i)] += mul(grad_low_t[h], weight.astype(bf16), 1, 0) + jnp.where(on, conv, 0.0)
                    here = [g[:, HALO:HALO + SUB] for g in around_g]
                    cross[h] += mul(jnp.concatenate(around_v, axis=0), jnp.concatenate(here, axis=0), 0, 0)
                return c

            lax.fori_loop(first, last, second_part, 0)
            scale = inv * root
            spread = [((small[2, h] + root * small[0, h]) * scale).astype(bf16) for h in every]
            spread += [((small[3, h] + root * small[1, h]) * scale).astype(bf16) for h in every]
            spread = jnp.concatenate(spread, axis=0)

            def spread_marks(i, c):
                t = token(i)
                member = ((t >= lo) & (t < hi)).astype(f32).astype(bf16)
                acc[:2 * width, lanes(i)] += mul(spread, member, 1, 0)
                return c

            lax.fori_loop(first, last, spread_marks, 0)

        return carry

    lax.fori_loop(0, len_ref.shape[0], per_slot, 0)
    sums_ref[...] = jnp.zeros_like(sums_ref)

    def store(i, c):
        at_lanes = pl.ds(pl.multiple_of(i * block, block), block)
        rounded = acc[:, at_lanes].astype(bf16)
        out_ref[:, at_lanes] = rounded
        sums_ref[...] += jnp.sum(rounded.astype(f32), axis=1, keepdims=True)
        return c

    lax.fori_loop(0, blocks, store, 0)
    low, high = HALO - taps // 2 - 16, HALO + SUB + taps // 2 + 16
    gap = (lax.broadcasted_iota(jnp.int32, (high - low, SUB), 0) + low
           - lax.broadcasted_iota(jnp.int32, (high - low, SUB), 1) - (HALO - taps // 2))
    for h in every:
        zone = cross[h, low:high, :]
        rows = [jnp.sum(jnp.where(gap == i, zone, 0.0), axis=0, keepdims=True) for i in range(taps)]
        conv_ref[h] = jnp.sum(jnp.concatenate(rows, axis=0), axis=1, keepdims=True)


def laid_taps(taps, half):
    heads, n = taps.shape
    room = 2 * SUB - (HALO - half) - (n - 1)
    return jnp.pad(taps[:, ::-1], ((0, 0), (room, 2 * SUB - room - n)))


def layout_of(lengths, bounds):
    lengths = lengths.astype(jnp.int32)
    starts = jnp.cumsum(lengths) - lengths
    upper = jnp.concatenate([bounds[:, 1:], lengths[:, None]], axis=1)
    lo = (bounds + starts[:, None]).reshape(-1, 1)
    hi = (upper + starts[:, None]).reshape(-1, 1)
    inv = 1.0 / jnp.maximum((upper - bounds).astype(f32), 1.0)
    return lengths, starts, lo, hi, inv


def specs(*kinds):
    return [pl.BlockSpec(memory_space=pltpu.SMEM if k == "s" else pltpu.VMEM) for k in kinds]


VMEM_LIMIT = 62 * 1024 * 1024


def attention_forward(layout, taps, qkv, blocks):
    lengths, starts, lo, hi, inv = layout
    slots, marks = inv.shape
    heads, n = taps.shape
    width, tokens = heads * HEAD_DIM, qkv.shape[1]
    shape = jax.ShapeDtypeStruct
    return pl.pallas_call(
        forward_kernel,
        name="attention_forward",
        out_shape=(
            shape((blocks, width, tokens // blocks), bf16),
            shape((slots, 2 * width, marks), f32),
            shape((slots, heads, marks, 1), f32),
            shape((slots, 4, heads, marks, marks), f32),
            shape((slots, PINV_ITERS, 4, heads, marks, marks), f32),
            shape((1, 1), f32),
        ),
        in_specs=specs("s", "s", "v", "v", "v", "v", "v"),
        out_specs=specs(*"vvvvvv"),
        scratch_shapes=[
            pltpu.VMEM((width, tokens + 2 * HALO), bf16),
            pltpu.VMEM((heads, 2 * SUB, SUB), bf16),
            pltpu.VMEM((2 * width, marks), f32),
        ],
        cost_estimate=pl.CostEstimate(flops=20_000_000_000, bytes_accessed=12_000_000, transcendentals=2_000_000),
        compiler_params=pltpu.CompilerParams(vmem_limit_bytes=VMEM_LIMIT),
    )(lengths, starts, lo, hi, inv, laid_taps(taps, n // 2), qkv)


def attention_backward(layout, taps, qkv, grad, saved):
    lengths, starts, lo, hi, inv = layout
    slots, marks = inv.shape
    heads, n = taps.shape
    width, tokens = heads * HEAD_DIM, qkv.shape[1]
    shape = jax.ShapeDtypeStruct
    return pl.pallas_call(
        backward_kernel,
        name="attention_backward",
        out_shape=(
            shape((3 * width, tokens), bf16),
            shape((3 * width, 1), f32),
            shape((heads, n, 1), f32),
        ),
        in_specs=specs(*"ssvvvvvvvvvv"),
        out_specs=specs(*"vvv"),
        scratch_shapes=[
            pltpu.VMEM((width, tokens + 2 * HALO), bf16),
            pltpu.VMEM((width, tokens + 2 * HALO), bf16),
            pltpu.VMEM((heads, 2 * SUB, SUB), bf16),
            pltpu.VMEM((3 * width, tokens), f32),
            pltpu.VMEM((4, heads, marks, marks), f32),
            pltpu.VMEM((heads, 2 * SUB, SUB), f32),
        ],
        cost_estimate=pl.CostEstimate(flops=50_000_000_000, bytes_accessed=18_000_000, transcendentals=2_000_000),
        compiler_params=pltpu.CompilerParams(vmem_limit_bytes=VMEM_LIMIT),
    )(lengths, starts, lo, hi, inv, laid_taps(taps[:, ::-1], n // 2), qkv, grad, *saved)


def layer_norm(row_data, gain_vec, shift_vec):
    centre = row_data - jnp.mean(row_data, axis=1, keepdims=True)
    spread = jnp.mean(centre * centre, axis=1, keepdims=True)
    return centre * lax.rsqrt(spread + norm_eps) * gain_vec[None, :] + shift_vec[None, :]


def gelu_exact(values):
    return jax.nn.gelu(values, approximate=False)


def widened(rows, width):
    return jnp.pad(rows, ((0, 0),) * (rows.ndim - 1) + ((0, width - rows.shape[-1]),))


def swap(x, mask):
    size = lax.axis_size("batch")
    return lax.ppermute(x, "batch", [(i, i ^ mask) for i in range(size)])


def joined(a, b):
    return (a.astype(f32) + b.astype(f32)).astype(bf16)


def bits_of(size):
    return [1 << k for k in range(size.bit_length() - 1)]


def place_of(size):
    if size == 1:
        return [0]
    return [((p & (size // 2 - 1)) << 1) | (p // (size // 2)) for p in range(size)]


def gather_relative(block, order, size):
    pieces = {0: block}
    for mask in order:
        pieces.update({key ^ mask: swap(piece, mask) for key, piece in list(pieces.items())})
    return [pieces[key] for key in place_of(size)]


def scatter_relative(pieces, order):
    for mask in order:
        pieces = {key: joined(piece, swap(pieces[key ^ mask], mask)) for key, piece in pieces.items() if not key & mask}
    return pieces[0]


def across_heads(x):
    return lax.all_to_all(x, "heads", 0, 0, tiled=True)


def sum_over_line(blocks):
    size = blocks.shape[0]
    here = lax.axis_index("heads")

    def pick(at):
        return lax.dynamic_index_in_dim(blocks, jnp.clip(at, 0, size - 1), 0, keepdims=False)

    up = down = None
    for k in range(1, size):
        send_up, send_down = pick(size - k + here), pick(k - size + here)
        if k > 1:
            send_up, send_down = joined(send_up, up), joined(send_down, down)
        up = lax.ppermute(send_up, "heads", [(h, h + 1) for h in range(k)])
        down = lax.ppermute(send_down, "heads", [(size - 1 - h, size - 2 - h) for h in range(k)])
    total = pick(here).astype(f32)
    return total if up is None else total + up.astype(f32) + down.astype(f32)


def body(
    tokens,
    qkv_weight,
    qv_bias,
    conv_weight,
    out_weight,
    out_bias,
    norm1_gain,
    norm1_bias,
    ffn_in_weight,
    ffn_in_bias,
    ffn_out_weight,
    ffn_out_bias,
    norm2_gain,
    norm2_bias,
    cotangent,
    seq_lengths,
    segment_ids,
    landmark_bounds,
):
    tok_count, model_width = tokens.shape
    head_width = qkv_weight.shape[2]
    heads_here = head_width // HEAD_DIM
    head_total, taps = conv_weight.shape
    groups, packs = lax.axis_size("heads"), lax.axis_size("batch")
    devices = groups * packs
    quarter = tok_count // groups
    ffn_own = ffn_in_bias.shape[0]
    ffn_all = ffn_own * devices
    head_index = lax.axis_index("heads")

    places = place_of(packs)
    bits = bits_of(packs)
    rising, falling = bits[1:] + bits[:1], bits[1:][::-1] + bits[:1]

    def shared(x):
        return across_heads(jnp.broadcast_to(x[None], (groups, *x.shape)))

    def whole_of(x, order):
        return jnp.concatenate(gather_relative(shared(x), order, packs), axis=0)

    whole_in = whole_of(ffn_in_weight.T, rising).reshape(ffn_all, model_width)
    whole_in_bias = whole_of(ffn_in_bias, falling).reshape(ffn_all)
    whole_out = whole_of(ffn_out_weight, falling).reshape(ffn_all, model_width)
    whole_attn = shared(out_weight).reshape(groups * head_width, model_width)

    layout = layout_of(seq_lengths, landmark_bounds)
    own_tokens = lax.dynamic_slice_in_dim(tokens, head_index * quarter, quarter, 0).astype(f32)
    conv_own = lax.dynamic_slice_in_dim(conv_weight, head_index * heads_here, heads_here, 0)
    qv_own = lax.dynamic_slice_in_dim(qv_bias, head_index * head_width, head_width, 1)
    flat_qkv = qkv_weight.reshape(model_width, 3 * head_width)
    bias_column = jnp.concatenate([qv_own[0], jnp.zeros_like(qv_own[0]), qv_own[1]])
    qkv = (
        lax.dot_general(flat_qkv, tokens, (((0,), (1,)), ((), ())), preferred_element_type=f32)
        + bias_column[:, None]
    ).astype(bf16)
    mixed, *saved, bound = attention_forward(layout, conv_own, qkv, groups)
    mixed = lax.all_to_all(mixed, "heads", 0, 0, tiled=True).reshape(groups * head_width, quarter)
    attn = lax.dot_general(mixed, whole_attn, contract_rows, preferred_element_type=f32)
    first_res = own_tokens + attn + out_bias[None, :]
    norm1_out, norm1_pull = jax.vjp(layer_norm, first_res, norm1_gain, norm1_bias)
    norm1_low = norm1_out.astype(bf16)
    pre_act = (
        lax.dot_general(norm1_low, whole_in, contract_cols, preferred_element_type=f32)
        + whole_in_bias.astype(f32)[None, :]
    )
    hidden_act, gelu_pull = jax.vjp(gelu_exact, pre_act)
    hidden_low = hidden_act.astype(bf16)
    ffn_result = jnp.dot(hidden_low, whole_out, preferred_element_type=f32) + ffn_out_bias[None, :]
    final_out, norm2_pull = jax.vjp(layer_norm, norm1_out + ffn_result, norm2_gain, norm2_bias)
    grad_second, grad_gain_two, grad_shift_two = norm2_pull(cotangent.astype(f32))
    grad_ffn_low = grad_second.astype(bf16)
    grad_ffn_bias = jnp.sum(grad_ffn_low.astype(f32), axis=0)

    def summed_to_owner(left, right, order):
        half = ffn_all // 2
        away = lax.dot_general(left[:, half:], right, contract_rows, preferred_element_type=f32).astype(bf16)
        away = swap(away, bits[0])
        kept = lax.dot_general(left[:, :half], right, contract_rows, preferred_element_type=f32)
        kept = (kept + away.astype(f32)).astype(bf16).reshape(packs // 2, groups, ffn_own, model_width)
        return scatter_relative({places[p]: kept[p] for p in range(packs // 2)}, order[:-1])

    down_block = summed_to_owner(hidden_low, grad_ffn_low, rising)
    grad_hidden = lax.dot_general(grad_ffn_low, whole_out, contract_cols, preferred_element_type=f32)
    grad_pre = gelu_pull(grad_hidden)[0].astype(bf16)
    grad_in_bias = jnp.sum(grad_pre.astype(f32), axis=0)
    up_block = summed_to_owner(grad_pre, norm1_low, falling)
    grad_norm1 = grad_second + jnp.dot(grad_pre, whole_in, preferred_element_type=f32)
    grad_first, grad_gain_one, grad_shift_one = norm1_pull(grad_norm1)
    grad_attn = grad_first.astype(bf16)
    grad_out_bias = jnp.sum(grad_attn.astype(f32), axis=0)
    grad_mix = lax.dot_general(whole_attn, grad_attn, contract_cols, preferred_element_type=f32).astype(bf16)
    grad_mix = lax.all_to_all(grad_mix.reshape(groups, head_width, quarter), "heads", 0, 0, tiled=True)
    out_part = lax.dot_general(
        grad_attn, mixed, (((0,), (1,)), ((), ())), preferred_element_type=f32
    ).astype(bf16)

    vector_all = jnp.stack(
        [grad_ffn_bias, grad_gain_two, grad_shift_two, grad_gain_one, grad_shift_one, grad_out_bias]
    )
    vector_own = model_width // devices
    pack_cols = model_width // packs
    live_slots = jnp.where(head_index == 0, jnp.sum((seq_lengths > 0).astype(f32)), 0.0)
    spot = [places.index(mask) for mask in range(packs)]
    absolute = jnp.asarray(spot, jnp.int32)[jnp.arange(packs) ^ lax.axis_index("batch")]
    extras = jnp.concatenate(
        [
            jnp.take(grad_in_bias.reshape(packs, groups, ffn_own), absolute, axis=0),
            jnp.transpose(vector_all.reshape(6, packs, groups, vector_own), (1, 2, 0, 3)).reshape(
                packs, groups, 6 * vector_own
            ),
            jnp.broadcast_to(jnp.stack([bound[0, 0], live_slots]), (packs, groups, 2)),
        ],
        axis=2,
    )
    extras = jnp.sum(lax.all_to_all(extras, "batch", 0, 0, tiled=True), axis=0)
    extra = jnp.sum(across_heads(extras), axis=0)
    out_block = lax.all_to_all(out_part.reshape(packs, pack_cols, model_width), "batch", 0, 0, tiled=True)
    out_block = jnp.sum(out_block.astype(f32), axis=0).astype(bf16)
    out_block = jnp.transpose(out_block.reshape(pack_cols, groups, head_width), (1, 0, 2))
    out_share = jnp.sum(across_heads(out_block).astype(f32), axis=0).T

    grad_qkv, row_sums, grad_conv = attention_backward(layout, conv_own, qkv, grad_mix, saved)
    qkv_part = lax.dot_general(
        tokens, grad_qkv, (((0,), (1,)), ((), ())), preferred_element_type=f32
    ).astype(bf16)
    input_part = lax.dot_general(
        grad_qkv, flat_qkv, (((0,), (1,)), ((), ())), preferred_element_type=f32
    ).astype(bf16)
    input_grad = grad_first + sum_over_line(input_part.reshape(groups, quarter, model_width))
    down_share = jnp.sum(across_heads(down_block).astype(f32), axis=0)
    up_share = jnp.sum(across_heads(up_block).astype(f32), axis=0).T
    sums = row_sums[:, 0]
    common = jnp.concatenate([sums[:head_width], sums[2 * head_width :], grad_conv.reshape(-1)])
    pack_rows = model_width // packs
    rows_qkv = -(-(pack_rows + 1) // 16) * 16
    qkv_send = jnp.concatenate(
        [
            qkv_part.reshape(packs, pack_rows, 3 * head_width),
            jnp.broadcast_to(widened(common[None], 3 * head_width).astype(bf16), (packs, 1, 3 * head_width)),
            jnp.zeros((packs, rows_qkv - pack_rows - 1, 3 * head_width), bf16),
        ],
        axis=1,
    )
    qkv_total = jnp.sum(lax.all_to_all(qkv_send, "batch", 0, 0, tiled=True).astype(f32), axis=0)
    common = qkv_total[pack_rows]
    at_bound = ffn_own + 6 * vector_own
    return (
        final_out.astype(bf16),
        input_grad,
        qkv_total[:pack_rows].reshape(pack_rows, 3, head_width),
        common[: 2 * head_width].reshape(2, head_width),
        common[2 * head_width : 2 * head_width + heads_here * taps].reshape(heads_here, taps),
        out_share,
        up_share,
        extra[:ffn_own],
        down_share,
        extra[ffn_own:at_bound].reshape(6, vector_own),
        extra[at_bound] / (extra[at_bound + 1] * head_total),
    )


def solution(mesh):
    in_specs = (
        P("batch", None),
        P(None, None, "heads"),
        P(),
        P(),
        P("heads", None),
        P(),
        P(),
        P(),
        P(None, ("batch", "heads")),
        P(("batch", "heads")),
        P(("batch", "heads"), None),
        P(),
        P(),
        P(),
        P(("batch", "heads"), None),
        P("batch"),
        P("batch"),
        P("batch", None),
    )
    out_specs = (
        P(("batch", "heads"), None),
        P(("batch", "heads"), None),
        P("batch", None, "heads"),
        P(None, "heads"),
        P("heads", None),
        P("heads", "batch"),
        P(None, ("batch", "heads")),
        P(("batch", "heads")),
        P(("batch", "heads"), None),
        P(None, ("batch", "heads")),
        P(),
    )
    return jax.shard_map(body, mesh=mesh, in_specs=in_specs, out_specs=out_specs, check_vma=False)
```
